32 devices in a mesh: group: 2 (over y), ctx: 4 (over z), head: 2 (over x), req: 2 (over core).
Axes of the slice: x: 2, y: 2, z: 4, core: 2. Of those that a mesh axis runs over, the one named last changes fastest.
Arguments:
- fresh_hidden: bfloat16 [4, 512, 8192], P(('group', 'req'), 'ctx', 'head'), parts along dimension 0, may hold values from -6 to 6
- latent_down: bfloat16 [8192, 512], P('head'), may hold values from -0.0625 to 0.0625
- cache_latents: bfloat16 [4, 1024, 512], P(('group', 'req'), 'ctx', 'head'), parts along dimension 0, may hold values from -6 to 6
- key_up: bfloat16 [2, 256, 128], P('head'), may hold values from -0.375 to 0.375
- value_up: bfloat16 [2, 256, 128], P('head'), may hold values from -0.375 to 0.375
- queries: bfloat16 [4, 512, 2048], P(('group', 'req'), 'ctx', 'head'), parts along dimension 0, may hold values from -160 to 160
- span_start: int32 [4, 4], P(('group', 'req')), parts along dimension 0, may hold values from 0 to 3, as said below
Outputs:
- attention: bfloat16 [4, 512, 2048], P(('group', 'req'), 'ctx', 'head'), parts along dimension 0
The draws below stay inside these ranges and needn't reach their ends.
There are 2 independent parts, one for each index of `group`. The reference program is written for one: setup_inputs(seed, part) draws one part's arguments, and reference() takes and returns one part's arrays. A program takes and returns all parts, laid end to end along the dimension named above; an argument that names none is the same for every part. Nothing has to cross between parts.
Inputs may be any that keep to these rules, and one draw needn't show every extreme that they name: For each request span_start is a permutation of 0 to 4 - 1 over the spans.
All inputs are finite; a program needn't handle non-finite values.
Results may differ from the reference program's by a relative error of at most 0.035.
Values may be sent and summed in bfloat16 or wider, within the bound.
No kernel may reach another device: no remote copies, remote signals or barrier semaphores. Data moves between devices by JAX's collectives and lax.ppermute only.
A program may use at most 128 MiB of HBM per device.

```python
import jax
import jax.numpy as jnp
from jax import lax

D = 8192
HD = 128
R = 256
GROUP_Q = 8
FRESH_DEV = 128
CACHE_DEV = 256
KVH = 2
QH = 16
REQS = 2
FRESH = 512
CACHE = 1024
SEQ = 1536
N_CTX = 4


def draw_queries(key, part):
    first_key = jax.random.fold_in(key, 0)
    result = jnp.clip(jax.random.normal(first_key, (REQS, FRESH, QH * HD), jnp.float32), -6.0, 6.0)
    return result.astype(jnp.bfloat16)


def draw_span_start(key, part):
    orders = jnp.stack([jax.random.permutation(jax.random.fold_in(key, 100 + index), N_CTX) for index in range(REQS)])
    return orders.astype(jnp.int32)


def block_scale(rng, shape, cuts, smallest, top_value):
    level, own = 1.0, jax.random.fold_in(rng, 6)
    for position, blocks in cuts:
        heights = jnp.exp(jax.random.uniform(jax.random.fold_in(own, position), (blocks,), jnp.float32, smallest / len(cuts), top_value / len(cuts)))
        level = level * jnp.repeat(heights, shape[position] // blocks).reshape([-1 if axis == position else 1 for axis in range(len(shape))])
    return level


def normal_values(key, dims, scale, bound, cuts=(), held_as=jnp.bfloat16):
    loudness = block_scale(key, dims, cuts, -0.22, 0.18) if cuts else 1.0
    values = jax.random.normal(key, dims, jnp.float32) * scale * loudness
    return jnp.minimum(jnp.maximum(values, -bound), bound).astype(held_as)


def setup_inputs(seed: int = 0, part: int = 0) -> dict:
    seeds = jax.random.split(jax.random.key(seed), 8)
    part_splits = jax.random.split(jax.random.fold_in(seeds[7], part), 8)
    return {
        "fresh_hidden": normal_values(part_splits[0], (REQS, FRESH, D), 1.0, 6.0, ((0, 2), (1, 4), (2, 2))),
        "latent_down": normal_values(seeds[1], (D, 2 * R), D ** -0.5, 0.0625, ((0, 2),)),
        "cache_latents": normal_values(part_splits[2], (REQS, CACHE, 2 * R), 1.0, 6.0, ((0, 2), (1, 4), (2, 2))),
        "key_up": normal_values(seeds[3], (KVH, R, HD), R ** -0.5, 0.375, ((0, 2),)),
        "value_up": normal_values(seeds[4], (KVH, R, HD), R ** -0.5, 0.375, ((0, 2),)),
        "queries": draw_queries(jax.random.fold_in(jax.random.fold_in(seeds[7], part), 71), part),
        "span_start": draw_span_start(jax.random.fold_in(jax.random.fold_in(seeds[7], part), 71), part),
    }


ROPE_BASE = 500000.0
SCORE_FLOOR = -1e30


def rotate(field, positions):
    half_dim = field.shape[-1] // 2
    inv_freq = ROPE_BASE ** (-(jnp.arange(half_dim, dtype=jnp.float32) * 2.0 / field.shape[-1]))
    angles = positions.astype(jnp.float32)[:, None] * inv_freq[None, :]
    cosine = jnp.cos(angles)
    sine_part = jnp.sin(angles)
    first_half = field[..., :half_dim]
    second_half = field[..., half_dim:]
    return jnp.concatenate([first_half * cosine - second_half * sine_part, second_half * cosine + first_half * sine_part], axis=-1)


def reference(fresh_hidden, latent_down, cache_latents, key_up, value_up, queries, span_start):
    score_scale = HD ** -0.5
    results = []
    for request in range(REQS):
        fresh_lat = jnp.dot(fresh_hidden[request], latent_down, preferred_element_type=jnp.float32).astype(jnp.bfloat16)
        latents = jnp.concatenate([cache_latents[request].reshape(N_CTX, CACHE_DEV, 2 * R), fresh_lat.reshape(N_CTX, FRESH_DEV, 2 * R)], axis=1).reshape(SEQ, 2 * R)
        places = span_start[request].astype(jnp.int32)
        cache_pos = places[:, None] * CACHE_DEV + jnp.arange(CACHE_DEV, dtype=jnp.int32)[None, :]
        fresh_pos = CACHE + places[:, None] * FRESH_DEV + jnp.arange(FRESH_DEV, dtype=jnp.int32)[None, :]
        key_pos = jnp.concatenate([cache_pos, fresh_pos], axis=1).reshape(SEQ)
        query_pos = fresh_pos.reshape(FRESH)
        visible = key_pos[None, :] <= query_pos[:, None]
        query_all = queries[request].reshape(FRESH, KVH, GROUP_Q, HD)

        def head_out(kv_index):
            key_rows = rotate(jnp.dot(latents[:, :R], key_up[kv_index], preferred_element_type=jnp.float32), key_pos).astype(jnp.bfloat16)
            value_rows = jnp.dot(latents[:, R:], value_up[kv_index], preferred_element_type=jnp.float32).astype(jnp.bfloat16)

            def one_query_head(member):
                rotated = rotate(query_all[:, kv_index, member, :].astype(jnp.float32), query_pos).astype(jnp.bfloat16)
                scores = jnp.dot(rotated, key_rows.T, preferred_element_type=jnp.float32) * score_scale
                scores = jnp.where(visible, scores, SCORE_FLOOR)
                row_max = jnp.max(scores, axis=1, keepdims=True)
                weights = jnp.where(visible, jnp.exp(scores - row_max), 0.0)
                row_sum = jnp.sum(weights, axis=1)
                mixed_out = jnp.dot(weights.astype(jnp.bfloat16), value_rows, preferred_element_type=jnp.float32) / row_sum[:, None]
                return mixed_out.astype(jnp.bfloat16)

            return lax.map(one_query_head, jnp.arange(GROUP_Q))

        per_head = lax.map(head_out, jnp.arange(KVH))
        results.append(per_head.transpose(2, 0, 1, 3).reshape(FRESH, QH * HD))
    return jnp.stack(results)
```

```python
import functools
import math

import jax
import jax.numpy as jnp
import numpy as np
from jax import lax
from jax.experimental import pallas as pl
from jax.experimental.pallas import tpu as pltpu
from jax.sharding import PartitionSpec as P

ROPE_BASE = 500000.0
SCORE_FLOOR = -1e30
VMEM_LIMIT = 24 * 1024 * 1024


def inverse_frequencies(head_dim):
    half = np.arange(head_dim // 2, dtype=np.float64)
    return np.tile(ROPE_BASE ** (-2.0 * half / head_dim), 2)


def half_signs(head_dim):
    return np.where(np.arange(head_dim) < head_dim // 2, -1.0, 1.0)


def offset_table(rows, head_dim):
    angles = np.arange(rows)[:, None] * inverse_frequencies(head_dim)[None, :]
    sines = np.sin(angles) * half_signs(head_dim)[None, :]
    return jnp.asarray(np.concatenate([np.cos(angles), sines], axis=0), jnp.float32)


def base_table(positions, head_dim):
    freq = jnp.asarray(inverse_frequencies(head_dim), jnp.float32)
    angles = positions.astype(jnp.float32)[:, None] * freq[None, :]
    sines = jnp.sin(angles) * jnp.asarray(half_signs(head_dim), jnp.float32)[None, :]
    return jnp.concatenate([jnp.cos(angles), sines], axis=0)


def rotation(base_ref, base_row, table_ref, rows):
    bases = base_ref.shape[0] // 2
    offsets = table_ref.shape[0] // 2
    base_cos = base_ref[base_row : base_row + 1, :]
    base_sin = base_ref[bases + base_row : bases + base_row + 1, :]
    off_cos = table_ref[:rows, :]
    off_sin = table_ref[offsets : offsets + rows, :]
    return (
        base_cos * off_cos - base_sin * off_sin,
        base_sin * off_cos + base_cos * off_sin,
    )


def rotate(field, cosine, sine):
    return field * cosine + pltpu.roll(field, field.shape[1] // 2, 1) * sine


def call(kernel, out_shape, operands, smem, flops, name):
    in_specs = [
        pl.BlockSpec(memory_space=pltpu.SMEM if index in smem else pltpu.VMEM)
        for index in range(len(operands))
    ]
    out_specs = jax.tree.map(lambda _: pl.BlockSpec(memory_space=pltpu.VMEM), out_shape)
    return pl.pallas_call(
        kernel,
        out_shape=out_shape,
        in_specs=in_specs,
        out_specs=out_specs,
        compiler_params=pltpu.CompilerParams(vmem_limit_bytes=VMEM_LIMIT),
        cost_estimate=pl.CostEstimate(
            flops=flops, bytes_accessed=flops // 256, transcendentals=0
        ),
        name=name,
    )(*operands)


def rebuild_rows(key_latents, value_latents, key_up, value_up, cosine, sine, out_ref):
    head_dim = key_up.shape[1]
    keys = jnp.dot(key_latents, key_up, preferred_element_type=jnp.float32)
    values = jnp.dot(value_latents, value_up, preferred_element_type=jnp.float32)
    out_ref[:, :head_dim] = rotate(keys, cosine, sine).astype(out_ref.dtype)
    out_ref[:, head_dim:] = values.astype(out_ref.dtype)


def rebuild_cached(own, other, own_is_key, base, base_row, table, key_up, value_up, name):
    def kernel(flag_ref, own_ref, other_ref, base_ref, table_ref, key_ref, value_ref, out_ref):
        is_key = jnp.full(own_ref.shape, flag_ref[0], jnp.int32) > 0
        own_rows, other_rows = own_ref[...], other_ref[...]
        key_latents = jnp.where(is_key, own_rows, other_rows)
        value_latents = jnp.where(is_key, other_rows, own_rows)
        cosine, sine = rotation(base_ref, base_row, table_ref, own_ref.shape[0])
        rebuild_rows(
            key_latents, value_latents, key_ref[...], value_ref[...], cosine, sine, out_ref
        )

    rows, head_dim = own.shape[0], key_up.shape[1]
    return call(
        kernel,
        jax.ShapeDtypeStruct((rows, 2 * head_dim), own.dtype),
        (own_is_key, own, other, base, table, key_up, value_up),
        (0,),
        4 * rows * own.shape[1] * head_dim,
        name,
    )


def rebuild_fresh(partial, received, base, base_row, table, key_up, value_up):
    def kernel(partial_ref, received_ref, base_ref, table_ref, key_ref, value_ref, out_ref):
        rank = key_ref.shape[0]
        latents = partial_ref[...].astype(jnp.float32) + received_ref[...].astype(jnp.float32)
        latents = latents.astype(out_ref.dtype)
        cosine, sine = rotation(base_ref, base_row, table_ref, out_ref.shape[0])
        rebuild_rows(
            latents[:, :rank], latents[:, rank:], key_ref[...], value_ref[...], cosine, sine, out_ref
        )

    rows, head_dim = partial.shape[0], key_up.shape[1]
    return call(
        kernel,
        jax.ShapeDtypeStruct((rows, 2 * head_dim), partial.dtype),
        (partial, received, base, table, key_up, value_up),
        (),
        4 * rows * key_up.shape[0] * head_dim,
        "rebuild_fresh",
    )


def absorb(query, blocks, limits_ref, limit_rows, peak, total):
    head_dim = query.shape[1]
    scores = []
    for block, row in zip(blocks, limit_rows):
        part = lax.dot_general(
            query, block[:, :head_dim], (((1,), (1,)), ((), ())), preferred_element_type=jnp.float32
        )
        if row is not None:
            ahead = lax.broadcasted_iota(jnp.int32, part.shape, 1) - lax.broadcasted_iota(
                jnp.int32, part.shape, 0
            )
            part = jnp.where(ahead <= limits_ref[row], part, SCORE_FLOOR)
        scores.append(part)
    top = functools.reduce(
        jnp.maximum, [jnp.max(part, axis=1, keepdims=True) for part in scores]
    )
    top = jnp.broadcast_to(top, (query.shape[0], head_dim))
    new_peak = top if peak is None else jnp.maximum(peak, top)
    added = None
    for part, block in zip(scores, blocks):
        copies = part.shape[1] // head_dim
        shift = new_peak if copies == 1 else jnp.concatenate([new_peak] * copies, axis=1)
        weights = jnp.exp2(part - shift).astype(block.dtype)
        values = jnp.concatenate(
            [block[:, head_dim:], jnp.ones((block.shape[0], head_dim), block.dtype)], axis=1
        )
        product = jnp.dot(weights, values, preferred_element_type=jnp.float32)
        added = product if added is None else added + product
    if total is not None:
        decay = jnp.exp2(peak - new_peak)
        added = added + total * jnp.concatenate([decay, decay], axis=1)
    return new_peak, added


def attend_own(queries, base, base_row, table, limits, limit_rows, blocks, head_dim):
    rows, width = queries.shape
    heads = width // head_dim
    scale = head_dim**-0.5 * math.log2(math.e)

    def kernel(limits_ref, query_ref, base_ref, table_ref, *refs):
        block_refs = refs[: len(blocks)]
        rotated_ref, peak_ref, total_ref = refs[len(blocks) :]
        cosine, sine = rotation(base_ref, base_row, table_ref, rows)
        cosine, sine = cosine * scale, sine * scale
        loaded = [ref[...] for ref in block_refs]
        for head in range(heads):
            lanes = slice(head * head_dim, (head + 1) * head_dim)
            query = rotate(query_ref[:, lanes].astype(jnp.float32), cosine, sine)
            query = query.astype(rotated_ref.dtype)
            rotated_ref[:, lanes] = query
            peak, total = absorb(query, loaded, limits_ref, limit_rows, None, None)
            peak_ref[head] = peak
            total_ref[head] = total

    keys = sum(block.shape[0] for block in blocks)
    return call(
        kernel,
        (
            jax.ShapeDtypeStruct((rows, width), queries.dtype),
            jax.ShapeDtypeStruct((heads, rows, head_dim), jnp.float32),
            jax.ShapeDtypeStruct((heads, rows, 2 * head_dim), jnp.float32),
        ),
        (limits, queries, base, table) + tuple(blocks),
        (0,),
        6 * rows * width * keys,
        "attend_own",
    )


def attend_more(state, limits, limit_rows, blocks, head_dim, last, name):
    rotated, peak, total = state
    rows, width = rotated.shape
    heads = width // head_dim

    def kernel(limits_ref, rotated_ref, peak_in, total_in, *refs):
        block_refs = refs[: len(blocks)]
        outs = refs[len(blocks) :]
        loaded = [ref[...] for ref in block_refs]
        for head in range(heads):
            lanes = slice(head * head_dim, (head + 1) * head_dim)
            new_peak, new_total = absorb(
                rotated_ref[:, lanes], loaded, limits_ref, limit_rows, peak_in[head], total_in[head]
            )
            if last:
                mixed = new_total[:, :head_dim] / new_total[:, head_dim:]
                outs[0][:, lanes] = mixed.astype(outs[0].dtype)
            else:
                outs[0][head] = new_peak
                outs[1][head] = new_total

    keys = sum(block.shape[0] for block in blocks)
    if last:
        out_shape = jax.ShapeDtypeStruct((rows, width), rotated.dtype)
    else:
        out_shape = (
            jax.ShapeDtypeStruct(peak.shape, peak.dtype),
            jax.ShapeDtypeStruct(total.shape, total.dtype),
        )
    result = call(
        kernel,
        out_shape,
        (limits, rotated, peak, total) + tuple(blocks),
        (0,),
        6 * rows * width * keys,
        name,
    )
    return result if last else (rotated,) + tuple(result)


def per_device(
    head_count, span_count, fresh_hidden, latent_down, cache_latents, key_up, value_up, queries, span_start
):
    key_up, value_up = key_up[0], value_up[0]
    head_dim = key_up.shape[1]
    rank = key_up.shape[0]
    cached = cache_latents[0]
    cache_dev = cached.shape[0]
    fresh_dev = queries.shape[1]
    cache_total = cache_dev * span_count
    head_id = lax.axis_index("head")
    span_id = lax.axis_index("ctx")

    def along(value, axis, size, step):
        return lax.ppermute(value, axis, [(i, (i + step) % size) for i in range(size)])

    def both_halves(own):
        if head_count == 2:
            return own, along(own, "head", 2, 1), (head_id == 0).astype(jnp.int32)[None]
        full = lax.all_gather(own, "head", axis=1, tiled=True)
        return full[:, :rank], full[:, rank:], jnp.ones((1,), jnp.int32)

    early = span_count // 2
    own_halves = both_halves(cached)
    early_own = along(cached, "ctx", span_count, early) if span_count > 1 else None

    partial = jnp.dot(fresh_hidden[0], latent_down, preferred_element_type=jnp.float32)
    partial = partial.astype(jnp.bfloat16)
    received = sum(along(partial, "head", head_count, step) for step in range(1, head_count))

    places = span_start[0]
    sources = (span_id - jnp.arange(span_count, dtype=jnp.int32)) % span_count
    source_places = places[sources]
    own_place = source_places[0]
    bases = jnp.stack(
        [
            cache_total + own_place * fresh_dev,
            own_place * cache_dev,
            source_places[early] * cache_dev,
        ]
    )
    base = base_table(bases, head_dim)
    table = offset_table(max(cache_dev, fresh_dev), head_dim)
    limits = (own_place - source_places) * fresh_dev

    own_cached = rebuild_cached(*own_halves, base, 1, table, key_up, value_up, "rebuild_own")
    own_fresh = rebuild_fresh(partial, received, base, 0, table, key_up, value_up)

    state = attend_own(
        queries[0], base, 0, table, limits, (None, 0), (own_cached, own_fresh), head_dim
    )
    more_cached, more_fresh, fresh_rows = [], [], []
    order = sorted(range(1, span_count), key=lambda step: (step != early, step))
    for step in order:
        if step == early:
            more_cached.append(
                rebuild_cached(
                    *both_halves(early_own), base, 2, table, key_up, value_up, "rebuild_early"
                )
            )
        else:
            more_cached.append(along(own_cached, "ctx", span_count, step))
    for step in order:
        more_fresh.append(along(own_fresh, "ctx", span_count, step))
        fresh_rows.append(step)
    state = attend_more(
        state, limits, (None,) * len(more_cached), more_cached, head_dim, False, "attend_cached"
    )
    mixed = attend_more(
        state, limits, tuple(fresh_rows), more_fresh, head_dim, True, "attend_fresh"
    )
    return mixed[None]


def solution(mesh):
    return jax.shard_map(
        functools.partial(per_device, mesh.shape["head"], mesh.shape["ctx"]),
        mesh=mesh,
        in_specs=(
            P(("group", "req"), "ctx", "head"),
            P("head", None),
            P(("group", "req"), "ctx", "head"),
            P("head", None, None),
            P("head", None, None),
            P(("group", "req"), "ctx", "head"),
            P(("group", "req"), None),
        ),
        out_specs=P(("group", "req"), "ctx", "head"),
        check_vma=False,
    )
```

```python
import functools
import math

import jax
import jax.numpy as jnp
import numpy as np
from jax import lax
from jax.experimental import pallas as pl
from jax.experimental.pallas import tpu as pltpu
from jax.sharding import PartitionSpec as P

ROPE_BASE = 500000.0
SCORE_FLOOR = -1e30
VMEM_LIMIT = 24 * 1024 * 1024
GROUP_OWN, GROUP_MORE, GROUP_LAST = 4, 4, 4


def inverse_frequencies(head_dim):
    half = np.arange(head_dim // 2, dtype=np.float64)
    return np.tile(ROPE_BASE ** (-2.0 * half / head_dim), 2)


def half_signs(head_dim):
    return np.where(np.arange(head_dim) < head_dim // 2, -1.0, 1.0)


def padded(rows):
    return -(-rows // 8) * 8


class Angles:
    def __init__(self, cache_dev, fresh_dev, span_count, head_dim):
        self.longest = padded(max(cache_dev, fresh_dev))
        self.places = padded(span_count)
        places = np.arange(self.places)
        firsts = (
            np.arange(self.longest),
            places * cache_dev,
            cache_dev * span_count + places * fresh_dev,
        )
        signs = half_signs(head_dim)[None, :]
        rows = []
        for positions in firsts:
            angles = positions[:, None] * inverse_frequencies(head_dim)[None, :]
            rows += [np.cos(angles), np.sin(angles) * signs]
        self.values = np.concatenate(rows, axis=0).astype(np.float32)

    def rotation(self, table_ref, fresh, place, rows):
        first = 2 * self.longest + (2 * self.places if fresh else 0)
        base_cos = table_ref[pl.ds(first + place, 1), :]
        base_sin = table_ref[pl.ds(first + self.places + place, 1), :]
        off_cos = table_ref[:rows, :]
        off_sin = table_ref[self.longest : self.longest + rows, :]
        return (
            base_cos * off_cos - base_sin * off_sin,
            base_sin * off_cos + base_cos * off_sin,
        )


def rotate(field, cosine, sine):
    return field * cosine + pltpu.roll(field, field.shape[1] // 2, 1) * sine


def place_of(places_ref, step):
    spans = places_ref.shape[1]
    return places_ref[0, lax.rem(lax.axis_index("ctx") + spans - step, spans)]


def call(kernel, out_shape, operands, flops, name, out_space=pltpu.VMEM, scratch=()):
    in_specs = [
        pl.BlockSpec(memory_space=pltpu.SMEM if index == 0 else pltpu.VMEM)
        for index in range(len(operands))
    ]
    out_specs = jax.tree.map(lambda _: pl.BlockSpec(memory_space=out_space), out_shape)
    return pl.pallas_call(
        kernel,
        out_shape=out_shape,
        in_specs=in_specs,
        out_specs=out_specs,
        scratch_shapes=list(scratch),
        compiler_params=pltpu.CompilerParams(vmem_limit_bytes=VMEM_LIMIT),
        cost_estimate=pl.CostEstimate(
            flops=flops, bytes_accessed=flops // 256, transcendentals=0
        ),
        name=name,
    )(*operands)


def rebuild_rows(key_latents, value_latents, key_up, value_up, cosine, sine, out_ref):
    head_dim = key_up.shape[1]
    keys = jnp.dot(key_latents, key_up, preferred_element_type=jnp.float32)
    values = jnp.dot(value_latents, value_up, preferred_element_type=jnp.float32)
    out_ref[:, :head_dim] = rotate(keys, cosine, sine).astype(out_ref.dtype)
    out_ref[:, head_dim:] = values.astype(out_ref.dtype)


def rebuild_cached(own, other, paired, places, step, angles, table, key_up, value_up, name):
    def kernel(places_ref, own_ref, other_ref, table_ref, key_ref, value_ref, out_ref):
        own_rows, other_rows = own_ref[...], other_ref[...]
        if paired:
            is_key = jnp.full(own_rows.shape, lax.axis_index("head"), jnp.int32) == 0
            key_latents = jnp.where(is_key, own_rows, other_rows)
            value_latents = jnp.where(is_key, other_rows, own_rows)
        else:
            key_latents, value_latents = own_rows, other_rows
        cosine, sine = angles.rotation(
            table_ref, False, place_of(places_ref, step), own_rows.shape[0]
        )
        rebuild_rows(
            key_latents, value_latents, key_ref[...], value_ref[...], cosine, sine, out_ref
        )

    rows, head_dim = own.shape[0], key_up.shape[1]
    return call(
        kernel,
        jax.ShapeDtypeStruct((rows, 2 * head_dim), own.dtype),
        (places, own, other, table, key_up, value_up),
        4 * rows * own.shape[1] * head_dim,
        name,
    )


def rebuild_fresh(partial, received, places, angles, table, key_up, value_up):
    def kernel(places_ref, partial_ref, received_ref, table_ref, key_ref, value_ref, out_ref):
        rank = key_ref.shape[0]
        latents = partial_ref[...].astype(jnp.float32) + received_ref[...].astype(jnp.float32)
        latents = latents.astype(out_ref.dtype)
        cosine, sine = angles.rotation(
            table_ref, True, place_of(places_ref, 0), out_ref.shape[0]
        )
        rebuild_rows(
            latents[:, :rank], latents[:, rank:], key_ref[...], value_ref[...], cosine, sine, out_ref
        )

    rows, head_dim = partial.shape[0], key_up.shape[1]
    return call(
        kernel,
        jax.ShapeDtypeStruct((rows, 2 * head_dim), partial.dtype),
        (places, partial, received, table, key_up, value_up),
        4 * rows * key_up.shape[0] * head_dim,
        "rebuild_fresh",
    )


def visibility(places_ref, step, rows, columns):
    limit = (place_of(places_ref, 0) - place_of(places_ref, step)) * columns
    ahead = lax.broadcasted_iota(jnp.int32, (rows, columns), 1) - lax.broadcasted_iota(
        jnp.int32, (rows, columns), 0
    )
    return jnp.where(ahead <= limit, 0.0, SCORE_FLOOR)


def absorb(query, blocks, hidden, peak, total):
    head_dim = query.shape[1]
    scores = []
    for block, bias in zip(blocks, hidden):
        part = lax.dot_general(
            query, block[:, :head_dim], (((1,), (1,)), ((), ())), preferred_element_type=jnp.float32
        )
        if bias is not None:
            heads = query.shape[0] // bias.shape[0]
            part = (part.reshape(heads, *bias.shape) + bias[None]).reshape(part.shape)
        scores.append(part)
    scores = scores[0] if len(scores) == 1 else jnp.concatenate(scores, axis=1)
    top = jnp.broadcast_to(jnp.max(scores, axis=1, keepdims=True), (query.shape[0], head_dim))
    new_peak = top if peak is None else jnp.maximum(peak, top)
    copies = scores.shape[1] // head_dim
    shift = new_peak if copies == 1 else jnp.concatenate([new_peak] * copies, axis=1)
    weights = jnp.exp2(scores - shift).astype(blocks[0].dtype)
    values = jnp.concatenate([block[:, head_dim:] for block in blocks], axis=0)
    values = jnp.concatenate([values, jnp.ones_like(values)], axis=1)
    added = jnp.dot(weights, values, preferred_element_type=jnp.float32)
    if total is not None:
        decay = jnp.exp2(peak - new_peak)
        added = added + total * jnp.concatenate([decay, decay], axis=1)
    return new_peak, added


def biases(places_ref, blocks, fresh_steps, rows):
    return [
        None if step is None else visibility(places_ref, step, rows, block.shape[0])
        for block, step in zip(blocks, fresh_steps)
    ]


def groups(heads, size):
    size = math.gcd(heads, size)
    return [range(start, start + size) for start in range(0, heads, size)]


def attend_own(queries, places, angles, table, fresh_steps, blocks, head_dim):
    rows, width = queries.shape
    heads = width // head_dim
    scale = head_dim**-0.5 * math.log2(math.e)

    def kernel(places_ref, query_ref, table_ref, *refs):
        block_refs = refs[: len(blocks)]
        rotated_ref, peak_ref, total_ref = refs[len(blocks) :]
        cosine, sine = angles.rotation(table_ref, True, place_of(places_ref, 0), rows)
        cosine, sine = cosine * scale, sine * scale
        loaded = [ref[...] for ref in block_refs]
        hidden = biases(places_ref, loaded, fresh_steps, rows)
        for group in groups(heads, GROUP_OWN):
            for head in group:
                query = query_ref[:, head * head_dim : (head + 1) * head_dim]
                query = rotate(query.astype(jnp.float32), cosine, sine)
                rotated_ref[head * rows : (head + 1) * rows, :] = query.astype(rotated_ref.dtype)
            span = slice(group.start * rows, group.stop * rows)
            peak, total = absorb(rotated_ref[span, :], loaded, hidden, None, None)
            peak_ref[span, :] = peak
            total_ref[span, :] = total

    keys = sum(block.shape[0] for block in blocks)
    return call(
        kernel,
        (
            jax.ShapeDtypeStruct((heads * rows, head_dim), queries.dtype),
            jax.ShapeDtypeStruct((heads * rows, head_dim), jnp.float32),
            jax.ShapeDtypeStruct((heads * rows, 2 * head_dim), jnp.float32),
        ),
        (places, queries, table) + tuple(blocks),
        6 * rows * width * keys,
        "attend_own",
    )


def attend_more(state, places, fresh_steps, blocks, rows, name):
    rotated, peak, total = state
    height, head_dim = rotated.shape

    def kernel(places_ref, rotated_ref, peak_in, total_in, *refs):
        loaded = [ref[...] for ref in refs[: len(blocks)]]
        peak_out, total_out = refs[len(blocks) :]
        hidden = biases(places_ref, loaded, fresh_steps, rows)
        for group in groups(height // rows, GROUP_MORE):
            span = slice(group.start * rows, group.stop * rows)
            peak_out[span, :], total_out[span, :] = absorb(
                rotated_ref[span, :], loaded, hidden, peak_in[span, :], total_in[span, :]
            )

    keys = sum(block.shape[0] for block in blocks)
    peak, total = call(
        kernel,
        (
            jax.ShapeDtypeStruct(peak.shape, peak.dtype),
            jax.ShapeDtypeStruct(total.shape, total.dtype),
        ),
        (places, rotated, peak, total) + tuple(blocks),
        6 * height * head_dim * keys,
        name,
    )
    return rotated, peak, total


def attend_last(state, places, fresh_steps, blocks, rows, name):
    rotated, peak, total = state
    height, head_dim = rotated.shape
    heads = height // rows
    plan = groups(heads, GROUP_LAST)

    def kernel(places_ref, rotated_ref, peak_in, total_in, *refs):
        loaded = [ref[...] for ref in refs[: len(blocks)]]
        out_ref, mixed_ref, sems = refs[len(blocks) :]
        hidden = biases(places_ref, loaded, fresh_steps, rows)
        copies = []
        for index, group in enumerate(plan):
            span = slice(group.start * rows, group.stop * rows)
            _, new_total = absorb(
                rotated_ref[span, :], loaded, hidden, peak_in[span, :], total_in[span, :]
            )
            mixed = new_total[:, :head_dim] / new_total[:, head_dim:]
            for place, head in enumerate(group):
                mixed_ref[:, head * head_dim : (head + 1) * head_dim] = mixed[
                    place * rows : (place + 1) * rows
                ].astype(mixed_ref.dtype)
            lanes = pl.ds(group.start * head_dim, len(group) * head_dim)
            copies.append(
                pltpu.make_async_copy(mixed_ref.at[:, lanes], out_ref.at[:, lanes], sems.at[index])
            )
            copies[-1].start()
        for copy in copies:
            copy.wait()

    keys = sum(block.shape[0] for block in blocks)
    shape = (rows, heads * head_dim)
    return call(
        kernel,
        jax.ShapeDtypeStruct(shape, rotated.dtype),
        (places, rotated, peak, total) + tuple(blocks),
        6 * height * head_dim * keys,
        name,
        out_space=pl.ANY,
        scratch=(pltpu.VMEM(shape, rotated.dtype), pltpu.SemaphoreType.DMA((len(plan),))),
    )


def per_device(
    head_count, span_count, fresh_hidden, latent_down, cache_latents, key_up, value_up, queries, span_start
):
    key_up, value_up = key_up[0], value_up[0]
    rank, head_dim = key_up.shape
    cached = cache_latents[0]
    cache_dev = cached.shape[0]
    fresh_dev = queries.shape[1]
    paired = head_count == 2

    def along(value, axis, size, step):
        return lax.ppermute(value, axis, [(i, (i + step) % size) for i in range(size)])

    def both_halves(own):
        if paired:
            return own, along(own, "head", 2, 1)
        full = lax.all_gather(own, "head", axis=1, tiled=True)
        return full[:, :rank], full[:, rank:]

    early = span_count // 2
    own_halves = both_halves(cached)
    early_own = along(cached, "ctx", span_count, early)

    partial = jnp.dot(fresh_hidden[0], latent_down, preferred_element_type=jnp.float32)
    partial = partial.astype(jnp.bfloat16)
    received = sum(along(partial, "head", head_count, step) for step in range(1, head_count))

    angles = Angles(cache_dev, fresh_dev, span_count, head_dim)
    table = jnp.asarray(angles.values)
    shared = (angles, table, key_up, value_up)
    own_cached = rebuild_cached(*own_halves, paired, span_start, 0, *shared, "rebuild_own")
    own_fresh = rebuild_fresh(partial, received, span_start, *shared)
    state = attend_own(
        queries[0], span_start, angles, table, (None, 0), (own_cached, own_fresh), head_dim
    )
    order = [early] + [step for step in range(1, span_count) if step != early]
    more_cached = [along(own_cached, "ctx", span_count, step) for step in order[1:]]
    early_cached = rebuild_cached(
        *both_halves(early_own), paired, span_start, early, *shared, "rebuild_early"
    )
    more_cached.insert(0, early_cached)
    more_fresh = [along(own_fresh, "ctx", span_count, step) for step in order]
    state = attend_more(
        state, span_start, (None,) * len(order), more_cached, fresh_dev, "attend_cached"
    )
    mixed = attend_last(state, span_start, tuple(order), more_fresh, fresh_dev, "attend_fresh")
    return mixed[None]


def solution(mesh):
    return jax.shard_map(
        functools.partial(per_device, mesh.shape["head"], mesh.shape["ctx"]),
        mesh=mesh,
        in_specs=(
            P(("group", "req"), "ctx", "head"),
            P("head", None),
            P(("group", "req"), "ctx", "head"),
            P("head", None, None),
            P("head", None, None),
            P(("group", "req"), "ctx", "head"),
            P(("group", "req"), None),
        ),
        out_specs=P(("group", "req"), "ctx", "head"),
        check_vma=False,
    )
```
